32 devices in a mesh: fx: 8 (over z, x), fy: 4 (over y, core).
Axes of the slice: x: 2, y: 2, z: 4, core: 2. Of those that a mesh axis runs over, the one named last changes fastest.
Arguments:
- loads: float32 [8, 4, 640, 384], P('fx', 'fy'), may hold values from -6 to 6
- schur: bfloat16 [8, 4, 640, 640], P('fx', 'fy')
- local_inverse: bfloat16 [8, 4, 640, 640], P('fx', 'fy')
- basis: bfloat16 [8, 4, 288, 640], P('fx', 'fy'), may hold values from -0.375 to 0.375
- coarse_inverse: bfloat16 [8, 4, 32, 1024], P(None, 'fy', None, 'fx'), may hold values from -0.25 to 0.25
- face_len: int32 [8, 4, 4], P('fx', 'fy'), may hold values from 80 to 160, as said below
Outputs:
- displacement: float32 [8, 4, 640, 384], P('fx', 'fy')
The draws below stay inside these ranges and needn't reach their ends.
Inputs may be any that keep to these rules, and one draw needn't show every extreme that they name: face_len[a, b, 0], [a, b, 1], [a, b, 2], [a, b, 3] are the live lengths of the west, east, south and north faces of subdomain (a, b); a shared face has one length: face_len[a, b, 1] == face_len[a, b + 1, 0] and face_len[a, b, 3] == face_len[a + 1, b, 2].
All inputs are finite; a program needn't handle non-finite values.
Results may differ from the reference program's by a relative error of at most 0.009.
Values may be sent and summed in bfloat16 or wider, within the bound.
No kernel may reach another device: no remote copies, remote signals or barrier semaphores. Data moves between devices by JAX's collectives and lax.ppermute only.
A program may use at most 64 MiB of HBM per device.

```python
import jax
import jax.numpy as jnp
from jax import lax

NI = 640
CD = 32
K = 384
ITERS = 2
SX = 8
SY = 4
NB = 288
NC = 1024


def definite(key, diag_lo, diag_hi, spread):
    jitter_key, diag_key = jax.random.split(key)
    extent = (SX, SY, NI, NI)
    jitter = jax.random.normal(jitter_key, extent, jnp.float32)
    jitter = jitter * (spread / (2.0 * NI) ** 0.5)
    symmetric = jitter + jnp.swapaxes(jitter, 2, 3)
    diagonal = jax.random.uniform(diag_key, (SX, SY, NI), jnp.float32, diag_lo, diag_hi)
    matrix = symmetric + diagonal[..., None] * jnp.eye(NI, dtype=jnp.float32)
    return matrix.astype(jnp.bfloat16)


def draw_schur(key, part):
    return definite(jax.random.fold_in(key, 11), 1.5, 3.0, 0.6)


def draw_local_inverse(key, part):
    return definite(jax.random.fold_in(key, 12), 0.45, 1.3, 0.18)


def draw_face_len(key, part):
    east_key, north_key = jax.random.split(jax.random.fold_in(key, 13))
    lowest = NI // 8
    highest = NI // 4
    across = jax.random.randint(east_key, (SX, SY + 1), lowest, highest + 1, jnp.int32)
    upward = jax.random.randint(north_key, (SX + 1, SY), lowest, highest + 1, jnp.int32)
    across = across.at[0, 0].set(highest)
    upward = upward.at[0, 0].set(lowest)
    return jnp.stack([across[:, :SY], across[:, 1:], upward[:SX], upward[1:]], axis=2)


def spiked(array, rng, source, target, shards_of, factor):
    owner, partner = [(jnp.arange(array.shape[position]) // (array.shape[position] // shards_of)).reshape([-1 if axis == position else 1 for axis in range(array.ndim)]) for position in (source, target)]
    chosen = jax.random.permutation(rng, shards_of)[partner]
    strong = (owner == chosen) | (owner == (partner + shards_of // 2) % shards_of)
    return jnp.where(strong, factor * array, array)


def levels(rng, shape, cuts, low, top_value):
    gain, own = 1.0, jax.random.fold_in(rng, 6)
    for dim, blocks in cuts:
        draws = jnp.exp(jax.random.uniform(jax.random.fold_in(own, dim), (blocks,), jnp.float32, low / len(cuts), top_value / len(cuts)))
        gain = gain * jnp.repeat(draws, shape[dim] // blocks).reshape([-1 if axis == dim else 1 for axis in range(len(shape))])
    return gain


def noise(stream_key, shape, deviation, reach, cuts=(), held_as=jnp.bfloat16):
    result = jax.random.normal(stream_key, shape, jnp.float32) * deviation
    if len(cuts) > 0:
        result = levels(stream_key, shape, cuts, -0.22, 0.18) * result
    return jnp.clip(result, min=-reach, max=reach).astype(held_as)


def bell_draw_with(key, dims, width, limit, shards, heavy, kind=jnp.bfloat16):
    array = width * jax.random.normal(key, dims, jnp.float32)
    if shards:
        array = array * levels(key, dims, shards, -0.22, 0.18)
    return jnp.clip(spiked(array, jax.random.fold_in(key, 3), *heavy), -limit, limit).astype(kind)


def setup_inputs(seed: int = 0) -> dict:
    splits = jax.random.split(jax.random.key(seed), 7)
    loads = noise(splits[0], (SX, SY, NI, K), 1.0, 6.0, ((0, 8), (1, 4)), jnp.float32)
    schur = draw_schur(jax.random.fold_in(splits[6], 71), 0)
    local_inverse = draw_local_inverse(jax.random.fold_in(splits[6], 71), 0)
    basis = noise(splits[3], (SX, SY, NB, NI), NB ** -0.5, 0.375, ((0, 8), (1, 4)))
    coarse_inverse = bell_draw_with(splits[4], (SX, SY, CD, NC), NC ** -0.5, 0.25, ((1, 4), (3, 8)), (1, 3, 4, 2.0))
    face_len = draw_face_len(jax.random.fold_in(splits[6], 71), 0)
    return {"loads": loads, "schur": schur, "local_inverse": local_inverse, "basis": basis, "coarse_inverse": coarse_inverse, "face_len": face_len}


damping = 0.7


def displace(field, row_step, col_step):
    padded = jnp.pad(field, ((1, 1), (1, 1)) + ((0, 0),) * (field.ndim - 2))
    return padded[1 - row_step:1 - row_step + SX, 1 - col_step:1 - col_step + SY]


def assemble(vector, live_mask):
    west_side = vector[:, :, 0]
    east_side = vector[:, :, 1]
    south_side = vector[:, :, 2]
    north_side = vector[:, :, 3]
    merged = jnp.stack([
        west_side + displace(east_side, 0, 1),
        east_side + displace(west_side, 0, -1),
        south_side + displace(north_side, 1, 0),
        north_side + displace(south_side, -1, 0)], axis=2)
    return merged * live_mask


def reference(loads, schur, local_inverse, basis, coarse_inverse, face_len):
    face_cells = NI // 4
    subdomains = SX * SY
    positions = lax.broadcasted_iota(jnp.int32, (SX, SY, 4, face_cells), 3)
    live_mask = (positions < face_len[:, :, :, None]).astype(jnp.float32)[..., None]
    row_index = lax.broadcasted_iota(jnp.int32, (SX, SY), 0)
    col_index = lax.broadcasted_iota(jnp.int32, (SX, SY), 1)
    shared = jnp.stack([col_index > 0, col_index < SY - 1, row_index > 0, row_index < SX - 1], axis=2)
    weights = jnp.where(shared, 0.5, 1.0).astype(jnp.float32)[:, :, :, None, None]
    local_load = loads.reshape(SX, SY, 4, face_cells, K)
    schur_flat = schur.reshape(subdomains, NI, NI)
    inverse_flat = local_inverse.reshape(subdomains, NI, NI)
    basis_flat = basis.reshape(subdomains, NB, NI)
    coarse_block = coarse_inverse.reshape(NC, NC)

    def precondition(residual):
        scaled = (weights * residual).astype(jnp.bfloat16).reshape(subdomains, NI, K)
        pieces = lax.map(lambda operands: jnp.dot(operands[0], operands[1], preferred_element_type=jnp.float32).astype(jnp.bfloat16), (basis_flat, scaled))
        pieces = pieces.reshape(SX, SY, 3, 3, CD, K).astype(jnp.float32)
        summed = jnp.zeros((SX, SY, CD, K), jnp.float32)
        for row_step in (-1, 0, 1):
            for col_step in (-1, 0, 1):
                summed = summed + displace(pieces[:, :, row_step + 1, col_step + 1], row_step, col_step)
        coarse_rhs = summed.astype(jnp.bfloat16).reshape(NC, K)
        coarse_sol = lax.dot_general(coarse_block, coarse_rhs, (((0,), (0,)), ((), ())), preferred_element_type=jnp.float32)
        coarse_sol = coarse_sol.astype(jnp.bfloat16).reshape(SX, SY, CD, K)
        nearby = jnp.stack([jnp.stack([displace(coarse_sol, -row_step, -col_step) for col_step in (-1, 0, 1)], axis=2) for row_step in (-1, 0, 1)], axis=2)
        nearby = nearby.reshape(subdomains, NB, K)

        def correct(operands):
            inverse_block, scaled_one, basis_block, nearby_one = operands
            local_part = jnp.dot(inverse_block, scaled_one, preferred_element_type=jnp.float32)
            coarse_part = lax.dot_general(basis_block, nearby_one, (((0,), (0,)), ((), ())), preferred_element_type=jnp.float32)
            return local_part + coarse_part

        correction = lax.map(correct, (inverse_flat, scaled, basis_flat, nearby))
        return correction.reshape(SX, SY, 4, face_cells, K)

    solution = jnp.zeros((SX, SY, 4, face_cells, K), jnp.float32)
    for sweep in range(ITERS):
        applied = lax.map(lambda operands: jnp.dot(operands[0], operands[1].astype(jnp.bfloat16), preferred_element_type=jnp.float32), (schur_flat, solution.reshape(subdomains, NI, K)))
        residual = assemble(local_load - applied.reshape(SX, SY, 4, face_cells, K), live_mask)
        solution = solution + damping * assemble(weights * precondition(residual), live_mask)
    return solution.reshape(SX, SY, NI, K)
```

```python
import jax
import jax.numpy as jnp
from jax import lax
from jax.sharding import PartitionSpec as P

damping = 0.7
wide_limit = 8 << 20


def swap(value, axis, flip):
    count = lax.axis_size(axis)
    return lax.ppermute(value, axis, [(i, i ^ flip) for i in range(count)])


def swap_odd(value, axis):
    count = lax.axis_size(axis)
    pairs = [(0, 0), (count - 1, count - 1)]
    for i in range(1, count - 1, 2):
        pairs += [(i, i + 1), (i + 1, i)]
    return lax.ppermute(value, axis, pairs)


def extended(block, sides, width):
    for axis, dim in sides:
        count = lax.axis_size(axis)
        forward = [(i, i + 1) for i in range(count - 1)]
        backward = [(target, source) for source, target in forward]
        low = lax.ppermute(
            lax.slice_in_dim(block, block.shape[dim] - width, None, axis=dim), axis, forward
        )
        high = lax.ppermute(lax.slice_in_dim(block, 0, width, axis=dim), axis, backward)
        block = jnp.concatenate([low, block, high], axis=dim)
    return block


def per_device(loads, schur, local_inverse, basis, coarse_inverse, face_len):
    local_dofs = loads.shape[2]
    load_cases = loads.shape[3]
    face_cells = local_dofs // 4
    basis_cols = basis.shape[2]
    coarse_dofs = basis_cols // 9
    row_index = lax.axis_index("fx")
    col_index = lax.axis_index("fy")
    row_count = lax.axis_size("fx")
    col_count = lax.axis_size("fy")
    row_width = col_count * coarse_dofs
    slice_cases = load_cases // col_count
    lengths = face_len[0, 0]
    positions = lax.broadcasted_iota(jnp.int32, (4, face_cells, 1), 1)
    live_mask = (positions < lengths[:, None, None]).astype(jnp.float32)
    shared = jnp.stack(
        [col_index > 0, col_index < col_count - 1, row_index > 0, row_index < row_count - 1]
    )[:, None, None]
    weights = jnp.where(shared, 0.5, 1.0).astype(jnp.float32)
    local_load = loads[0, 0].reshape(4, face_cells, load_cases)
    schur_block = schur[0, 0]
    inverse_block = local_inverse[0, 0]
    basis_block = basis[0, 0]
    bf16 = jnp.bfloat16
    f32 = jnp.float32
    row_odd = row_index % 2
    col_odd = col_index % 2

    def face(vector, which):
        return lax.dynamic_index_in_dim(vector, which, 0, keepdims=False).astype(bf16)

    def neighbours(vector):
        first_col = swap(face(vector, 1 - col_odd), "fy", 1)
        second_col = swap_odd(face(vector, col_odd), "fy")
        second_row = swap_odd(face(vector, 2 + row_odd), "fx")
        first_row = swap(face(vector, 3 - row_odd), "fx", 1)
        picked = [
            jnp.where(col_odd == 1, first_col, second_col),
            jnp.where(col_odd == 1, second_col, first_col),
            jnp.where(row_odd == 1, first_row, second_row),
            jnp.where(row_odd == 1, second_row, first_row),
        ]
        return jnp.where(shared, jnp.stack(picked).astype(f32), 0.0)

    def assemble(vector):
        return live_mask * (vector + neighbours(vector))

    wide = row_count * row_width * 9 * row_width * 2 <= wide_limit
    framed_basis = jnp.zeros((3, col_count + 2, coarse_dofs, local_dofs), bf16)
    framed_basis = lax.dynamic_update_slice(
        framed_basis,
        basis_block.reshape(3, 3, coarse_dofs, local_dofs),
        (0, col_index, 0, 0),
    )
    row_basis = framed_basis[:, 1:-1].reshape(3 * row_width, local_dofs)

    if wide:
        own = coarse_inverse[:, 0]
        even_part = swap(own, "fx", 1)
        odd_part = swap_odd(own, "fx")
        below = jnp.where(row_odd == 1, even_part, odd_part)
        above = jnp.where(row_odd == 1, odd_part, even_part)
        below = jnp.where(row_index > 0, below, 0)
        above = jnp.where(row_index < row_count - 1, above, 0)
        targets = jnp.concatenate([below, own, above], axis=2)
        sources = jnp.zeros((row_count + 2, row_width, 3 * row_width), bf16)
        for flip in range(col_count):
            part = swap(targets, "fy", flip) if flip else targets
            sources = lax.dynamic_update_slice(
                sources, part, (1, (col_index ^ flip) * coarse_dofs, 0)
            )
        operator = jnp.concatenate(
            [
                lax.dynamic_slice_in_dim(sources, row_index ^ flip, 3, 0).reshape(
                    3 * row_width, 3 * row_width
                )
                for flip in range(row_count)
            ],
            axis=0,
        )

        def coarse(scaled):
            pieces = lax.dot_general(
                scaled, row_basis, (((0,), (1,)), ((), ())), preferred_element_type=f32
            ).astype(bf16)

            def cases(which):
                return lax.dynamic_slice_in_dim(pieces, which * slice_cases, slice_cases, 0)

            total = cases(col_index).astype(f32)
            for flip in range(1, col_count):
                total = total + swap(cases(col_index ^ flip), "fy", flip).astype(f32)
            total = total.astype(bf16)
            rows = [total] + [swap(total, "fx", flip) for flip in range(1, row_count)]
            solved = jnp.dot(
                jnp.concatenate(rows, axis=1), operator, preferred_element_type=f32
            ).astype(bf16)
            whole = jnp.zeros((load_cases, 3 * row_width), bf16)
            for flip in range(col_count):
                part = swap(solved, "fy", flip) if flip else solved
                whole = lax.dynamic_update_slice(
                    whole, part, ((col_index ^ flip) * slice_cases, 0)
                )
            return lax.dot_general(
                row_basis, whole, (((0,), (1,)), ((), ())), preferred_element_type=f32
            )

    else:
        coarse_block = coarse_inverse.reshape(
            coarse_inverse.shape[0] * coarse_inverse.shape[2], coarse_inverse.shape[3]
        )

        def coarse(scaled):
            pieces = jnp.dot(basis_block, scaled, preferred_element_type=f32).astype(bf16)
            pieces = pieces.reshape(3, 3, coarse_dofs, load_cases)
            padded = extended(pieces, (("fx", 0), ("fy", 1)), 1)
            summed = padded[0::2, 0::2].astype(f32).sum(axis=(0, 1))
            coarse_rhs = summed.astype(bf16)
            partial_sol = lax.dot_general(
                coarse_block,
                lax.all_gather(coarse_rhs, "fx", axis=0, tiled=True),
                (((0,), (0,)), ((), ())),
                preferred_element_type=f32,
            )
            whole = lax.psum(partial_sol, "fy").astype(bf16)
            whole = whole.reshape(col_count, coarse_dofs, load_cases)
            framed = jnp.pad(whole, ((1, 1), (0, 0), (0, 0)))
            window = lax.dynamic_slice_in_dim(framed, col_index, 3, 0)
            nearby = extended(window[None], (("fx", 0),), 1)
            return lax.dot_general(
                basis_block,
                nearby.reshape(basis_cols, load_cases),
                (((0,), (0,)), ((), ())),
                preferred_element_type=f32,
            )

    def precondition(residual):
        scaled = (weights * residual).astype(bf16).reshape(local_dofs, load_cases)
        local_part = jnp.dot(inverse_block, scaled, preferred_element_type=f32)
        return (local_part + coarse(scaled)).reshape(4, face_cells, load_cases)

    residual = assemble(local_load)
    solution = damping * assemble(weights * precondition(residual))
    applied = jnp.dot(
        schur_block,
        solution.reshape(local_dofs, load_cases).astype(bf16),
        preferred_element_type=f32,
    )
    residual = assemble(local_load - applied.reshape(4, face_cells, load_cases))
    solution = solution + damping * assemble(weights * precondition(residual))
    return solution.reshape(1, 1, local_dofs, load_cases)


def solution(mesh):
    placed = (
        P("fx", "fy", None, None),
        P("fx", "fy", None, None),
        P("fx", "fy", None, None),
        P("fx", "fy", None, None),
        P(None, "fy", None, "fx"),
        P("fx", "fy", None),
    )
    return jax.shard_map(
        per_device, mesh=mesh, in_specs=placed, out_specs=P("fx", "fy", None, None), check_vma=False
    )
```

```python
import functools

import jax
import jax.numpy as jnp
from jax import lax
from jax.experimental import pallas as pl
from jax.experimental.pallas import tpu as pltpu
from jax.sharding import PartitionSpec as P

damping = 0.7
wide_limit = 8 << 20
bf16 = jnp.bfloat16
f32 = jnp.float32


def extended(block, sides, width):
    for axis, dim in sides:
        count = lax.axis_size(axis)
        forward = [(i, i + 1) for i in range(count - 1)]
        backward = [(target, source) for source, target in forward]
        low = lax.ppermute(
            lax.slice_in_dim(block, block.shape[dim] - width, None, axis=dim), axis, forward
        )
        high = lax.ppermute(lax.slice_in_dim(block, 0, width, axis=dim), axis, backward)
        block = jnp.concatenate([low, block, high], axis=dim)
    return block


def narrow_plan(loads, schur, local_inverse, basis, coarse_inverse, face_len):
    local_dofs = loads.shape[2]
    load_cases = loads.shape[3]
    face_cells = local_dofs // 4
    basis_cols = basis.shape[2]
    coarse_dofs = basis_cols // 9
    row_index = lax.axis_index("fx")
    col_index = lax.axis_index("fy")
    row_count = lax.axis_size("fx")
    col_count = lax.axis_size("fy")
    lengths = face_len[0, 0]
    positions = lax.broadcasted_iota(jnp.int32, (4, face_cells, 1), 1)
    live_mask = (positions < lengths[:, None, None]).astype(jnp.float32)
    shared = jnp.stack(
        [col_index > 0, col_index < col_count - 1, row_index > 0, row_index < row_count - 1]
    )
    weights = jnp.where(shared, 0.5, 1.0).astype(jnp.float32)[:, None, None]
    local_load = loads[0, 0].reshape(4, face_cells, load_cases)
    schur_block = schur[0, 0]
    inverse_block = local_inverse[0, 0]
    basis_block = basis[0, 0]
    coarse_block = coarse_inverse.reshape(
        coarse_inverse.shape[0] * coarse_inverse.shape[2], coarse_inverse.shape[3]
    )

    def assemble(vector):
        row_sides = extended(vector[2:4], (("fx", 0),), 1)
        col_sides = extended(vector[0:2], (("fy", 0),), 1)
        merged = jnp.stack(
            [
                vector[0] + col_sides[0],
                vector[1] + col_sides[3],
                vector[2] + row_sides[0],
                vector[3] + row_sides[3],
            ]
        )
        return merged * live_mask

    def accumulate(gathered):
        return lax.dot_general(
            coarse_block, gathered, (((0,), (0,)), ((), ())), preferred_element_type=jnp.float32
        )

    def precondition(residual):
        scaled = (weights * residual).astype(jnp.bfloat16).reshape(local_dofs, load_cases)
        pieces = jnp.dot(basis_block, scaled, preferred_element_type=jnp.float32).astype(
            jnp.bfloat16
        )
        pieces = pieces.reshape(3, 3, coarse_dofs, load_cases)
        padded = extended(pieces, (("fx", 0), ("fy", 1)), 1)
        summed = padded[0::2, 0::2].astype(jnp.float32).sum(axis=(0, 1))
        coarse_rhs = summed.astype(jnp.bfloat16)
        partial_sol = accumulate(lax.all_gather(coarse_rhs, "fx", axis=0, tiled=True))
        whole = lax.psum(partial_sol, "fy").astype(jnp.bfloat16)
        whole = whole.reshape(col_count, coarse_dofs, load_cases)
        framed = jnp.pad(whole, ((1, 1), (0, 0), (0, 0)))
        window = lax.dynamic_slice_in_dim(framed, col_index, 3, 0)
        nearby = extended(window[None], (("fx", 0),), 1)
        local_part = jnp.dot(inverse_block, scaled, preferred_element_type=jnp.float32)
        coarse_part = lax.dot_general(
            basis_block,
            nearby.reshape(basis_cols, load_cases),
            (((0,), (0,)), ((), ())),
            preferred_element_type=jnp.float32,
        )
        return (local_part + coarse_part).reshape(4, face_cells, load_cases)

    residual = assemble(local_load)
    solution = damping * assemble(weights * precondition(residual))
    applied = jnp.dot(
        schur_block,
        solution.reshape(local_dofs, load_cases).astype(jnp.bfloat16),
        preferred_element_type=jnp.float32,
    )
    residual = assemble(local_load - applied.reshape(4, face_cells, load_cases))
    solution = solution + damping * assemble(weights * precondition(residual))
    return solution.reshape(1, 1, local_dofs, load_cases)


def swap(value, axis, flip):
    count = lax.axis_size(axis)
    return lax.ppermute(value, axis, [(i, i ^ flip) for i in range(count)])


def swap_odd(value, axis):
    count = lax.axis_size(axis)
    pairs = [(0, 0), (count - 1, count - 1)]
    for i in range(1, count - 1, 2):
        pairs += [(i, i + 1), (i + 1, i)]
    return lax.ppermute(value, axis, pairs)


def local_kernel(body, outs, flops, *operands, scratch=(), name):
    size = sum(x.size * x.dtype.itemsize for x in operands)
    size += sum(x.size * x.dtype.itemsize for x in outs)
    specs = [
        pl.BlockSpec(memory_space=pltpu.SMEM if x.dtype == jnp.int32 else pltpu.VMEM)
        for x in operands
    ]
    return pl.pallas_call(
        body,
        out_shape=outs,
        in_specs=specs,
        out_specs=[pl.BlockSpec(memory_space=pltpu.VMEM)] * len(outs),
        scratch_shapes=scratch,
        compiler_params=pltpu.CompilerParams(vmem_limit_bytes=16 << 20),
        cost_estimate=pl.CostEstimate(flops=flops, bytes_accessed=size, transcendentals=0),
        name=name,
    )(*operands)


def grid_place():
    row, col = lax.axis_index("fx"), lax.axis_index("fy")
    shared = (
        col > 0,
        col < lax.axis_size("fy") - 1,
        row > 0,
        row < lax.axis_size("fx") - 1,
    )
    return row, col, shared


def weight_of(shared):
    return jnp.where(shared, 0.5, 1.0).astype(f32)


def incoming(side, received):
    row, col, shared = grid_place()
    odd = (col % 2 if side < 2 else row % 2) == 1
    first, second = received[:2] if side < 2 else received[2:]
    if side % 2 == 0:
        first, second = second, first
    picked = jnp.where(odd, second[...], first[...]).astype(f32)
    return jnp.where(shared[side], picked, 0.0)


def live(side, lengths, cells, cases):
    return lax.broadcasted_iota(jnp.int32, (cells, cases), 0) < lengths[side]


def assembled(side, value, received, lengths):
    total = value + incoming(side, received)
    return jnp.where(live(side, lengths, *value.shape), total, 0.0)


def put_faces(source, faces, cells):
    row, col, _ = grid_place()
    which = (1 - col % 2, col % 2, 2 + row % 2, 3 - row % 2)
    for face, index in zip(faces, which):
        start = pl.multiple_of(index * cells, cells)
        face[...] = source[pl.ds(start, cells), :].astype(bf16)


def basis_body(basis, framed, turned, *, coarse_dofs, col_count):
    _, col, _ = grid_place()
    width = col_count * coarse_dofs
    framed[...] = jnp.zeros_like(framed)
    for i in range(3):
        for j in range(3):
            column = col + j - 1

            @pl.when(jnp.logical_and(column >= 0, column < col_count))
            def _():
                start = pl.multiple_of(i * width + column * coarse_dofs, coarse_dofs)
                source = (i * 3 + j) * coarse_dofs
                framed[pl.ds(start, coarse_dofs), :] = basis[source : source + coarse_dofs, :]

    turned[...] = framed[...].T


def pieces_body(lengths, value, c1, c2, r2, r1, framed, scaled, *rest, cells):
    *parts, whole = rest
    _, col, shared = grid_place()
    received = (c1, c2, r1, r2)
    for side in range(4):
        rows = slice(side * cells, (side + 1) * cells)
        total = assembled(side, value[rows, :], received, lengths)
        scaled[rows, :] = (weight_of(shared[side]) * total).astype(bf16)
    whole[...] = lax.dot_general(
        scaled[...], framed[...], (((0,), (1,)), ((), ())), preferred_element_type=f32
    ).astype(bf16)
    size = parts[0].shape[0]
    for flip, part in enumerate(parts):
        part[...] = whole[pl.ds(pl.multiple_of((col ^ flip) * size, size), size), :]


def coarse_body(*refs):
    *rows, operator, solved = refs
    depth = rows[0].shape[1]
    total = None
    for index, row in enumerate(rows):
        part = jnp.dot(
            row[...], operator[index * depth : (index + 1) * depth, :], preferred_element_type=f32
        )
        total = part if total is None else total + part
    solved[...] = total.astype(bf16)


def correct_body(*refs, cells, parts):
    solved = refs[:parts]
    turned, local_part, weighted, c1, c2, r2, r1, whole = refs[parts:]
    _, col, shared = grid_place()
    size = solved[0].shape[0]
    for flip, part in enumerate(solved):
        whole[pl.ds(pl.multiple_of((col ^ flip) * size, size), size), :] = part[...]
    for side in range(4):
        rows = slice(side * cells, (side + 1) * cells)
        coarse_part = lax.dot_general(
            turned[rows, :], whole[...], (((1,), (1,)), ((), ())), preferred_element_type=f32
        )
        weighted[rows, :] = weight_of(shared[side]) * (local_part[rows, :] + coarse_part)
    put_faces(weighted, (c1, c2, r2, r1), cells)


def schur_body(
    lengths, weighted, c1, c2, r2, r1, schur, loads, moved, value, o1, o2, o3, o4, low, *, cells
):
    received = (c1, c2, r1, r2)
    for side in range(4):
        rows = slice(side * cells, (side + 1) * cells)
        moved[rows, :] = damping * assembled(side, weighted[rows, :], received, lengths)
        low[rows, :] = moved[rows, :].astype(bf16)
    value[...] = loads[...] - jnp.dot(schur[...], low[...], preferred_element_type=f32)
    put_faces(value, (o1, o2, o3, o4), cells)


def final_body(lengths, weighted, c1, c2, r2, r1, before, moved, *, cells):
    received = (c1, c2, r1, r2)
    for side in range(4):
        rows = slice(side * cells, (side + 1) * cells)
        total = assembled(side, weighted[rows, :], received, lengths)
        moved[rows, :] = before[rows, :] + damping * total


def wide_plan(loads, schur, local_inverse, basis, coarse_inverse, face_len):
    local_dofs = loads.shape[2]
    load_cases = loads.shape[3]
    cells = local_dofs // 4
    coarse_dofs = basis.shape[2] // 9
    row, col, shared = grid_place()
    row_count = lax.axis_size("fx")
    col_count = lax.axis_size("fy")
    width = col_count * coarse_dofs
    slice_cases = load_cases // col_count
    lengths = face_len.reshape(4)
    local_load = loads[0, 0]
    array = jax.ShapeDtypeStruct
    vector32 = array((local_dofs, load_cases), f32)
    vector16 = array((local_dofs, load_cases), bf16)
    face16 = [array((cells, load_cases), bf16)] * 4
    row16 = array((slice_cases, 3 * width), bf16)

    def exchange(faces):
        return (
            swap(faces[0], "fy", 1),
            swap_odd(faces[1], "fy"),
            swap_odd(faces[2], "fx"),
            swap(faces[3], "fx", 1),
        )

    whole_load = local_load.reshape(4, cells, load_cases)
    load_faces = [
        lax.dynamic_index_in_dim(whole_load, which, 0, keepdims=False).astype(bf16)
        for which in (1 - col % 2, col % 2, 2 + row % 2, 3 - row % 2)
    ]
    received = exchange(load_faces)

    framed, turned = local_kernel(
        functools.partial(basis_body, coarse_dofs=coarse_dofs, col_count=col_count),
        [array((3 * width, local_dofs), bf16), array((local_dofs, 3 * width), bf16)],
        0,
        basis[0, 0],
        name="frame",
    )

    own = coarse_inverse[:, 0]
    even_part = swap(own, "fx", 1)
    odd_part = swap_odd(own, "fx")
    below = jnp.where(row % 2 == 1, even_part, odd_part)
    above = jnp.where(row % 2 == 1, odd_part, even_part)
    below = jnp.where(shared[2], below, 0)
    above = jnp.where(shared[3], above, 0)
    targets = jnp.concatenate([below, own, above], axis=2)
    sources = jnp.zeros((row_count + 2, width, 3 * width), bf16)
    for flip in range(col_count):
        part = swap(targets, "fy", flip) if flip else targets
        sources = lax.dynamic_update_slice(sources, part, (1, (col ^ flip) * coarse_dofs, 0))
    operator = jnp.concatenate(
        [
            lax.dynamic_slice_in_dim(sources, row ^ flip, 3, 0).reshape(3 * width, 3 * width)
            for flip in range(row_count)
        ],
        axis=0,
    )

    def precondition(value, received):
        scaled, *parts = local_kernel(
            functools.partial(pieces_body, cells=cells),
            [vector16] + [row16] * col_count,
            2 * local_dofs * load_cases * 3 * width,
            lengths,
            value,
            *received,
            framed,
            scratch=[pltpu.VMEM((load_cases, 3 * width), bf16)],
            name="pieces",
        )
        total = parts[0].astype(f32)
        for flip in range(1, col_count):
            total = total + swap(parts[flip], "fy", flip).astype(f32)
        total = total.astype(bf16)
        rows = [total] + [swap(total, "fx", flip) for flip in range(1, row_count)]
        local_part = jnp.dot(local_inverse[0, 0], scaled, preferred_element_type=f32)
        (solved,) = local_kernel(
            coarse_body,
            [row16],
            2 * slice_cases * 9 * width * width * row_count,
            *rows,
            operator,
            name="coarse",
        )
        solved = [solved] + [swap(solved, "fy", flip) for flip in range(1, col_count)]
        weighted, *faces = local_kernel(
            functools.partial(correct_body, cells=cells, parts=col_count),
            [vector32] + face16,
            2 * local_dofs * load_cases * 3 * width,
            *solved,
            turned,
            local_part,
            scratch=[pltpu.VMEM((load_cases, 3 * width), bf16)],
            name="correct",
        )
        return weighted, exchange(faces)

    weighted, received = precondition(local_load, received)
    moved, value, *faces = local_kernel(
        functools.partial(schur_body, cells=cells),
        [vector32, vector32] + face16,
        2 * local_dofs * local_dofs * load_cases,
        lengths,
        weighted,
        *received,
        schur[0, 0],
        local_load,
        scratch=[pltpu.VMEM((local_dofs, load_cases), bf16)],
        name="schur",
    )
    weighted, received = precondition(value, exchange(faces))
    (moved,) = local_kernel(
        functools.partial(final_body, cells=cells),
        [vector32],
        8 * local_dofs * load_cases,
        lengths,
        weighted,
        *received,
        moved,
        name="final",
    )
    return moved.reshape(1, 1, local_dofs, load_cases)


def per_device(loads, schur, local_inverse, basis, coarse_inverse, face_len):
    row_count = lax.axis_size("fx")
    width = lax.axis_size("fy") * (basis.shape[2] // 9)
    wide = row_count * width * 9 * width * 2 <= wide_limit
    plan = wide_plan if wide else narrow_plan
    return plan(loads, schur, local_inverse, basis, coarse_inverse, face_len)


def solution(mesh):
    placed = (
        P("fx", "fy", None, None),
        P("fx", "fy", None, None),
        P("fx", "fy", None, None),
        P("fx", "fy", None, None),
        P(None, "fy", None, "fx"),
        P("fx", "fy", None),
    )
    return jax.shard_map(
        per_device, mesh=mesh, in_specs=placed, out_specs=P("fx", "fy", None, None), check_vma=False
    )
```

```python
import functools

import jax
import jax.numpy as jnp
from jax import lax
from jax.experimental import pallas as pl
from jax.experimental.pallas import tpu as pltpu
from jax.sharding import PartitionSpec as P

damping = 0.7
wide_limit = 8 << 20
bf16 = jnp.bfloat16
f32 = jnp.float32


def extended(block, sides, width):
    for axis, dim in sides:
        count = lax.axis_size(axis)
        forward = [(i, i + 1) for i in range(count - 1)]
        backward = [(target, source) for source, target in forward]
        low = lax.ppermute(
            lax.slice_in_dim(block, block.shape[dim] - width, None, axis=dim), axis, forward
        )
        high = lax.ppermute(lax.slice_in_dim(block, 0, width, axis=dim), axis, backward)
        block = jnp.concatenate([low, block, high], axis=dim)
    return block


def narrow_plan(loads, schur, local_inverse, basis, coarse_inverse, face_len):
    local_dofs = loads.shape[2]
    load_cases = loads.shape[3]
    face_cells = local_dofs // 4
    basis_cols = basis.shape[2]
    coarse_dofs = basis_cols // 9
    row_index = lax.axis_index("fx")
    col_index = lax.axis_index("fy")
    row_count = lax.axis_size("fx")
    col_count = lax.axis_size("fy")
    lengths = face_len[0, 0]
    positions = lax.broadcasted_iota(jnp.int32, (4, face_cells, 1), 1)
    live_mask = (positions < lengths[:, None, None]).astype(jnp.float32)
    shared = jnp.stack(
        [col_index > 0, col_index < col_count - 1, row_index > 0, row_index < row_count - 1]
    )
    weights = jnp.where(shared, 0.5, 1.0).astype(jnp.float32)[:, None, None]
    local_load = loads[0, 0].reshape(4, face_cells, load_cases)
    schur_block = schur[0, 0]
    inverse_block = local_inverse[0, 0]
    basis_block = basis[0, 0]
    coarse_block = coarse_inverse.reshape(
        coarse_inverse.shape[0] * coarse_inverse.shape[2], coarse_inverse.shape[3]
    )

    def assemble(vector):
        row_sides = extended(vector[2:4], (("fx", 0),), 1)
        col_sides = extended(vector[0:2], (("fy", 0),), 1)
        merged = jnp.stack(
            [
                vector[0] + col_sides[0],
                vector[1] + col_sides[3],
                vector[2] + row_sides[0],
                vector[3] + row_sides[3],
            ]
        )
        return merged * live_mask

    def accumulate(gathered):
        return lax.dot_general(
            coarse_block, gathered, (((0,), (0,)), ((), ())), preferred_element_type=jnp.float32
        )

    def precondition(residual):
        scaled = (weights * residual).astype(jnp.bfloat16).reshape(local_dofs, load_cases)
        pieces = jnp.dot(basis_block, scaled, preferred_element_type=jnp.float32).astype(
            jnp.bfloat16
        )
        pieces = pieces.reshape(3, 3, coarse_dofs, load_cases)
        padded = extended(pieces, (("fx", 0), ("fy", 1)), 1)
        summed = padded[0::2, 0::2].astype(jnp.float32).sum(axis=(0, 1))
        coarse_rhs = summed.astype(jnp.bfloat16)
        partial_sol = accumulate(lax.all_gather(coarse_rhs, "fx", axis=0, tiled=True))
        whole = lax.psum(partial_sol, "fy").astype(jnp.bfloat16)
        whole = whole.reshape(col_count, coarse_dofs, load_cases)
        framed = jnp.pad(whole, ((1, 1), (0, 0), (0, 0)))
        window = lax.dynamic_slice_in_dim(framed, col_index, 3, 0)
        nearby = extended(window[None], (("fx", 0),), 1)
        local_part = jnp.dot(inverse_block, scaled, preferred_element_type=jnp.float32)
        coarse_part = lax.dot_general(
            basis_block,
            nearby.reshape(basis_cols, load_cases),
            (((0,), (0,)), ((), ())),
            preferred_element_type=jnp.float32,
        )
        return (local_part + coarse_part).reshape(4, face_cells, load_cases)

    residual = assemble(local_load)
    solution = damping * assemble(weights * precondition(residual))
    applied = jnp.dot(
        schur_block,
        solution.reshape(local_dofs, load_cases).astype(jnp.bfloat16),
        preferred_element_type=jnp.float32,
    )
    residual = assemble(local_load - applied.reshape(4, face_cells, load_cases))
    solution = solution + damping * assemble(weights * precondition(residual))
    return solution.reshape(1, 1, local_dofs, load_cases)


def swap(value, axis, flip):
    count = lax.axis_size(axis)
    return lax.ppermute(value, axis, [(i, i ^ flip) for i in range(count)])


def swap_odd(value, axis):
    count = lax.axis_size(axis)
    pairs = [(0, 0), (count - 1, count - 1)]
    for i in range(1, count - 1, 2):
        pairs += [(i, i + 1), (i + 1, i)]
    return lax.ppermute(value, axis, pairs)


def shift(value, axis, step):
    count = lax.axis_size(axis)
    return lax.ppermute(value, axis, [(i, (i + step) % count) for i in range(count)])


def local_kernel(body, outs, flops, *operands, scratch=(), name):
    size = sum(x.size * x.dtype.itemsize for x in operands)
    size += sum(x.size * x.dtype.itemsize for x in outs)
    specs = [
        pl.BlockSpec(memory_space=pltpu.SMEM if x.dtype == jnp.int32 else pltpu.VMEM)
        for x in operands
    ]
    return pl.pallas_call(
        body,
        out_shape=outs,
        in_specs=specs,
        out_specs=[pl.BlockSpec(memory_space=pltpu.VMEM)] * len(outs),
        scratch_shapes=scratch,
        compiler_params=pltpu.CompilerParams(vmem_limit_bytes=16 << 20),
        cost_estimate=pl.CostEstimate(flops=flops, bytes_accessed=size, transcendentals=0),
        name=name,
    )(*operands)


def grid_place():
    row, col = lax.axis_index("fx"), lax.axis_index("fy")
    shared = (
        col > 0,
        col < lax.axis_size("fy") - 1,
        row > 0,
        row < lax.axis_size("fx") - 1,
    )
    return row, col, shared


def weight_of(shared):
    return jnp.where(shared, 0.5, 1.0).astype(f32)


def live(side, lengths, cells, cases):
    return lax.broadcasted_iota(jnp.int32, (cells, cases), 0) < lengths[side]


def assembled(side, value, received, lengths):
    shared = grid_place()[2][side]
    total = value + jnp.where(shared, received[side][...].astype(f32), 0.0)
    return jnp.where(live(side, lengths, *value.shape), total, 0.0)


def put_faces(source, faces, cells):
    for side, face in enumerate(faces):
        face[...] = source[side * cells : (side + 1) * cells, :].astype(bf16)


def faces_body(source, *faces):
    put_faces(source, faces, faces[0].shape[0])


def basis_body(basis, framed, turned, *, coarse_dofs, col_count):
    _, col, _ = grid_place()
    width = col_count * coarse_dofs
    framed[...] = jnp.zeros_like(framed)
    for i in range(3):
        for j in range(3):
            column = col + j - 1

            @pl.when(jnp.logical_and(column >= 0, column < col_count))
            def _():
                start = pl.multiple_of(i * width + column * coarse_dofs, coarse_dofs)
                source = (i * 3 + j) * coarse_dofs
                framed[pl.ds(start, coarse_dofs), :] = basis[source : source + coarse_dofs, :]

    turned[...] = framed[...].T


def pieces_body(lengths, value, w, e, s, n, framed, scaled, *rest, cells):
    *parts, whole = rest
    _, col, shared = grid_place()
    received = (w, e, s, n)
    for side in range(4):
        rows = slice(side * cells, (side + 1) * cells)
        total = assembled(side, value[rows, :], received, lengths)
        scaled[rows, :] = (weight_of(shared[side]) * total).astype(bf16)
    whole[...] = lax.dot_general(
        scaled[...], framed[...], (((0,), (1,)), ((), ())), preferred_element_type=f32
    ).astype(bf16)
    size = parts[0].shape[0]
    for flip, part in enumerate(parts):
        part[...] = whole[pl.ds(pl.multiple_of((col ^ flip) * size, size), size), :]


def pair_body(own, other, summed):
    row, _, _ = grid_place()
    odd = row % 2 == 1
    width = own.shape[1] // 3
    low = jnp.where(odd, other[...], own[...]).astype(f32)
    high = jnp.where(odd, own[...], other[...]).astype(f32)
    summed[:, :width] = low[:, :width].astype(bf16)
    summed[:, width : 3 * width] = (low[:, width:] + high[:, : 2 * width]).astype(bf16)
    summed[:, 3 * width :] = high[:, 2 * width :].astype(bf16)


def coarse_body(*refs):
    *rows, operator, solved = refs
    depth = rows[0].shape[1]
    total = None
    for index, row in enumerate(rows):
        part = jnp.dot(
            row[...], operator[index * depth : (index + 1) * depth, :], preferred_element_type=f32
        )
        total = part if total is None else total + part
    solved[...] = total.astype(bf16)


def correct_body(*refs, cells, parts):
    solved = refs[:parts]
    turned, local_part, weighted, *faces, whole = refs[parts:]
    _, col, shared = grid_place()
    size = solved[0].shape[0]
    for flip, part in enumerate(solved):
        whole[pl.ds(pl.multiple_of((col ^ flip) * size, size), size), :] = part[...]
    for side in range(4):
        rows = slice(side * cells, (side + 1) * cells)
        coarse_part = lax.dot_general(
            turned[rows, :], whole[...], (((1,), (1,)), ((), ())), preferred_element_type=f32
        )
        weighted[rows, :] = weight_of(shared[side]) * (local_part[rows, :] + coarse_part)
    put_faces(weighted, faces, cells)


def schur_body(
    lengths, weighted, w, e, s, n, schur, loads, moved, value, o1, o2, o3, o4, low, *, cells
):
    received = (w, e, s, n)
    for side in range(4):
        rows = slice(side * cells, (side + 1) * cells)
        moved[rows, :] = damping * assembled(side, weighted[rows, :], received, lengths)
        low[rows, :] = moved[rows, :].astype(bf16)
    value[...] = loads[...] - jnp.dot(schur[...], low[...], preferred_element_type=f32)
    put_faces(value, (o1, o2, o3, o4), cells)


def final_body(lengths, weighted, w, e, s, n, before, moved, *, cells):
    received = (w, e, s, n)
    for side in range(4):
        rows = slice(side * cells, (side + 1) * cells)
        total = assembled(side, weighted[rows, :], received, lengths)
        moved[rows, :] = before[rows, :] + damping * total


def wide_plan(loads, schur, local_inverse, basis, coarse_inverse, face_len):
    local_dofs = loads.shape[2]
    load_cases = loads.shape[3]
    cells = local_dofs // 4
    coarse_dofs = basis.shape[2] // 9
    row, col, shared = grid_place()
    row_count = lax.axis_size("fx")
    col_count = lax.axis_size("fy")
    width = col_count * coarse_dofs
    slice_cases = load_cases // col_count
    lengths = face_len.reshape(4)
    local_load = loads[0, 0]
    array = jax.ShapeDtypeStruct
    vector32 = array((local_dofs, load_cases), f32)
    vector16 = array((local_dofs, load_cases), bf16)
    face16 = [array((cells, load_cases), bf16)] * 4
    row16 = array((slice_cases, 3 * width), bf16)

    def exchange(faces):
        west, east, south, north = faces
        from_west = shift(east, "fy", 1)
        from_east = shift(west, "fy", -1)
        from_south = shift(north, "fx", 1)
        from_north = shift(south, "fx", -1)
        return from_west, from_east, from_south, from_north

    faces = local_kernel(faces_body, face16, local_dofs * load_cases, local_load, name="faces")
    received = exchange(faces)

    framed, turned = local_kernel(
        functools.partial(basis_body, coarse_dofs=coarse_dofs, col_count=col_count),
        [array((3 * width, local_dofs), bf16), array((local_dofs, 3 * width), bf16)],
        0,
        basis[0, 0],
        name="frame",
    )

    def gathered_inverse(own):
        even_part = swap(own, "fx", 1)
        odd_part = swap_odd(own, "fx")
        below = jnp.where(row % 2 == 1, even_part, odd_part)
        above = jnp.where(row % 2 == 1, odd_part, even_part)
        below = jnp.where(shared[2], below, 0)
        above = jnp.where(shared[3], above, 0)
        targets = jnp.concatenate([below, own, above], axis=2)
        sources = jnp.zeros((row_count + 2, width, 3 * width), bf16)
        for flip in range(col_count):
            part = swap(targets, "fy", flip) if flip else targets
            sources = lax.dynamic_update_slice(sources, part, (1, (col ^ flip) * coarse_dofs, 0))
        pair = row // 2
        pairs = row_count // 2
        blocks = [
            lax.dynamic_slice_in_dim(sources, 2 * ((pair - step + pairs) % pairs), 4, 0)
            for step in range(pairs)
        ]
        return jnp.concatenate([x.reshape(4 * width, 3 * width) for x in blocks], axis=0)

    def project(value, received):
        return local_kernel(
            functools.partial(pieces_body, cells=cells),
            [vector16] + [row16] * col_count,
            2 * local_dofs * load_cases * 3 * width,
            lengths,
            value,
            *received,
            framed,
            scratch=[pltpu.VMEM((load_cases, 3 * width), bf16)],
            name="pieces",
        )

    def precondition(scaled, parts, operator):
        total = parts[0].astype(f32)
        for flip in range(1, col_count):
            total = total + swap(parts[flip], "fy", flip).astype(f32)
        total = total.astype(bf16)
        (pair_sum,) = local_kernel(
            pair_body,
            [array((slice_cases, 4 * width), bf16)],
            4 * slice_cases * width,
            total,
            swap(total, "fx", 1),
            name="pair",
        )
        rows = [pair_sum] + [shift(pair_sum, "fx", 2 * k) for k in range(1, row_count // 2)]
        local_part = jnp.dot(local_inverse[0, 0], scaled, preferred_element_type=f32)
        (solved,) = local_kernel(
            coarse_body,
            [row16],
            12 * slice_cases * width * width * row_count,
            *rows,
            operator,
            name="coarse",
        )
        solved = [solved] + [swap(solved, "fy", flip) for flip in range(1, col_count)]
        weighted, *faces = local_kernel(
            functools.partial(correct_body, cells=cells, parts=col_count),
            [vector32] + face16,
            2 * local_dofs * load_cases * 3 * width,
            *solved,
            turned,
            local_part,
            scratch=[pltpu.VMEM((load_cases, 3 * width), bf16)],
            name="correct",
        )
        return weighted, exchange(faces)

    scaled, *parts = project(local_load, received)
    own, parts = lax.optimization_barrier((coarse_inverse[:, 0], parts))
    operator = gathered_inverse(own)
    weighted, received = precondition(scaled, parts, operator)
    moved, value, *faces = local_kernel(
        functools.partial(schur_body, cells=cells),
        [vector32, vector32] + face16,
        2 * local_dofs * local_dofs * load_cases,
        lengths,
        weighted,
        *received,
        schur[0, 0],
        local_load,
        scratch=[pltpu.VMEM((local_dofs, load_cases), bf16)],
        name="schur",
    )
    scaled, *parts = project(value, exchange(faces))
    weighted, received = precondition(scaled, parts, operator)
    (moved,) = local_kernel(
        functools.partial(final_body, cells=cells),
        [vector32],
        8 * local_dofs * load_cases,
        lengths,
        weighted,
        *received,
        moved,
        name="final",
    )
    return moved.reshape(1, 1, local_dofs, load_cases)


def per_device(loads, schur, local_inverse, basis, coarse_inverse, face_len):
    row_count = lax.axis_size("fx")
    width = lax.axis_size("fy") * (basis.shape[2] // 9)
    wide = row_count * width * 9 * width * 2 <= wide_limit
    plan = wide_plan if wide else narrow_plan
    return plan(loads, schur, local_inverse, basis, coarse_inverse, face_len)


def solution(mesh):
    placed = (
        P("fx", "fy", None, None),
        P("fx", "fy", None, None),
        P("fx", "fy", None, None),
        P("fx", "fy", None, None),
        P(None, "fy", None, "fx"),
        P("fx", "fy", None),
    )
    return jax.shard_map(
        per_device, mesh=mesh, in_specs=placed, out_specs=P("fx", "fy", None, None), check_vma=False
    )
```

```python
import functools

import jax
import jax.numpy as jnp
from jax import lax
from jax.experimental import pallas as pl
from jax.experimental.pallas import tpu as pltpu
from jax.sharding import PartitionSpec as P


damping = 0.7
wide_limit = 8 << 20
bf16 = jnp.bfloat16
f32 = jnp.float32


def extended(block, sides, width):
    for axis, dim in sides:
        count = lax.axis_size(axis)
        forward = [(i, i + 1) for i in range(count - 1)]
        backward = [(target, source) for source, target in forward]
        low = lax.ppermute(
            lax.slice_in_dim(block, block.shape[dim] - width, None, axis=dim), axis, forward
        )
        high = lax.ppermute(lax.slice_in_dim(block, 0, width, axis=dim), axis, backward)
        block = jnp.concatenate([low, block, high], axis=dim)
    return block


def narrow_plan(loads, schur, local_inverse, basis, coarse_inverse, face_len):
    local_dofs = loads.shape[2]
    load_cases = loads.shape[3]
    face_cells = local_dofs // 4
    basis_cols = basis.shape[2]
    coarse_dofs = basis_cols // 9
    row_index = lax.axis_index("fx")
    col_index = lax.axis_index("fy")
    row_count = lax.axis_size("fx")
    col_count = lax.axis_size("fy")
    lengths = face_len[0, 0]
    positions = lax.broadcasted_iota(jnp.int32, (4, face_cells, 1), 1)
    live_mask = (positions < lengths[:, None, None]).astype(jnp.float32)
    shared = jnp.stack(
        [col_index > 0, col_index < col_count - 1, row_index > 0, row_index < row_count - 1]
    )
    weights = jnp.where(shared, 0.5, 1.0).astype(jnp.float32)[:, None, None]
    local_load = loads[0, 0].reshape(4, face_cells, load_cases)
    schur_block = schur[0, 0]
    inverse_block = local_inverse[0, 0]
    basis_block = basis[0, 0]
    coarse_block = coarse_inverse.reshape(
        coarse_inverse.shape[0] * coarse_inverse.shape[2], coarse_inverse.shape[3]
    )

    def assemble(vector):
        row_sides = extended(vector[2:4], (("fx", 0),), 1)
        col_sides = extended(vector[0:2], (("fy", 0),), 1)
        merged = jnp.stack(
            [
                vector[0] + col_sides[0],
                vector[1] + col_sides[3],
                vector[2] + row_sides[0],
                vector[3] + row_sides[3],
            ]
        )
        return merged * live_mask

    def accumulate(gathered):
        return lax.dot_general(
            coarse_block, gathered, (((0,), (0,)), ((), ())), preferred_element_type=jnp.float32
        )

    def precondition(residual):
        scaled = (weights * residual).astype(jnp.bfloat16).reshape(local_dofs, load_cases)
        pieces = jnp.dot(basis_block, scaled, preferred_element_type=jnp.float32).astype(
            jnp.bfloat16
        )
        pieces = pieces.reshape(3, 3, coarse_dofs, load_cases)
        padded = extended(pieces, (("fx", 0), ("fy", 1)), 1)
        summed = padded[0::2, 0::2].astype(jnp.float32).sum(axis=(0, 1))
        coarse_rhs = summed.astype(jnp.bfloat16)
        partial_sol = accumulate(lax.all_gather(coarse_rhs, "fx", axis=0, tiled=True))
        whole = lax.psum(partial_sol, "fy").astype(jnp.bfloat16)
        whole = whole.reshape(col_count, coarse_dofs, load_cases)
        framed = jnp.pad(whole, ((1, 1), (0, 0), (0, 0)))
        window = lax.dynamic_slice_in_dim(framed, col_index, 3, 0)
        nearby = extended(window[None], (("fx", 0),), 1)
        local_part = jnp.dot(inverse_block, scaled, preferred_element_type=jnp.float32)
        coarse_part = lax.dot_general(
            basis_block,
            nearby.reshape(basis_cols, load_cases),
            (((0,), (0,)), ((), ())),
            preferred_element_type=jnp.float32,
        )
        return (local_part + coarse_part).reshape(4, face_cells, load_cases)

    residual = assemble(local_load)
    solution = damping * assemble(weights * precondition(residual))
    applied = jnp.dot(
        schur_block,
        solution.reshape(local_dofs, load_cases).astype(jnp.bfloat16),
        preferred_element_type=jnp.float32,
    )
    residual = assemble(local_load - applied.reshape(4, face_cells, load_cases))
    solution = solution + damping * assemble(weights * precondition(residual))
    return solution.reshape(1, 1, local_dofs, load_cases)


def swap(value, axis, flip):
    return lax.ppermute(value, axis, [(i, i ^ flip) for i in range(lax.axis_size(axis))])


def shift(value, axis, step):
    count = lax.axis_size(axis)
    return lax.ppermute(value, axis, [(i, (i + step) % count) for i in range(count)])


def local_kernel(body, outs, flops, *operands, scratch=()):
    size = sum(x.size * x.dtype.itemsize for x in operands)
    size += sum(x.size * x.dtype.itemsize for x in outs)
    specs = [
        pl.BlockSpec(memory_space=pltpu.SMEM if x.dtype == jnp.int32 else pltpu.VMEM)
        for x in operands
    ]
    return pl.pallas_call(
        body,
        out_shape=outs,
        in_specs=specs,
        out_specs=[pl.BlockSpec(memory_space=pltpu.VMEM)] * len(outs),
        scratch_shapes=scratch,
        compiler_params=pltpu.CompilerParams(vmem_limit_bytes=16 << 20),
        cost_estimate=pl.CostEstimate(flops=flops, bytes_accessed=size, transcendentals=0),
    )(*operands)


def grid_place():
    row, col = lax.axis_index("fx"), lax.axis_index("fy")
    shared = (
        col > 0,
        col < lax.axis_size("fy") - 1,
        row > 0,
        row < lax.axis_size("fx") - 1,
    )
    return row, col, shared


def weight_of(shared):
    return jnp.where(shared, 0.5, 1.0).astype(f32)


def assembled(side, value, received, mask, rows):
    shared = grid_place()[2][side]
    total = value + jnp.where(shared, received[side][...].astype(f32), 0.0)
    lanes = mask.shape[1]
    return total * jnp.concatenate([mask[rows, :]] * (value.shape[1] // lanes), axis=1)


def put_faces(source, faces, cells):
    for side, face in enumerate(faces):
        face[...] = source[side * cells : (side + 1) * cells, :].astype(bf16)


def faces_body(lengths, source, *outs):
    *faces, mask = outs
    cells = faces[0].shape[0]
    put_faces(source, faces, cells)
    shape = (cells, mask.shape[1])
    for side in range(4):
        live = lax.broadcasted_iota(jnp.int32, shape, 0) < lengths[side]
        mask[side * cells : (side + 1) * cells, :] = live.astype(f32)


def basis_body(basis, framed, turned, *, coarse_dofs, col_count):
    _, col, _ = grid_place()
    width = col_count * coarse_dofs
    framed[...] = jnp.zeros_like(framed)
    for i in range(3):
        for j in range(3):
            column = col + j - 1

            @pl.when(jnp.logical_and(column >= 0, column < col_count))
            def _():
                start = pl.multiple_of(i * width + column * coarse_dofs, coarse_dofs)
                source = (i * 3 + j) * coarse_dofs
                framed[pl.ds(start, coarse_dofs), :] = basis[source : source + coarse_dofs, :]

    turned[...] = framed[...].T


def pieces_body(mask, value, w, e, s, n, framed, scaled, *rest, cells):
    *parts, whole = rest
    _, col, shared = grid_place()
    received = (w, e, s, n)
    for side in range(4):
        rows = slice(side * cells, (side + 1) * cells)
        total = assembled(side, value[rows, :], received, mask, rows)
        scaled[rows, :] = (weight_of(shared[side]) * total).astype(bf16)
    whole[...] = lax.dot_general(
        scaled[...], framed[...], (((0,), (1,)), ((), ())), preferred_element_type=f32
    ).astype(bf16)
    size = parts[0].shape[0]
    for flip, part in enumerate(parts):
        part[...] = whole[pl.ds(pl.multiple_of((col ^ flip) * size, size), size), :]


def pair_body(own, other, summed):
    row, _, _ = grid_place()
    odd = row % 2 == 1
    width = own.shape[1] // 3
    low = jnp.where(odd, other[...], own[...]).astype(f32)
    high = jnp.where(odd, own[...], other[...]).astype(f32)
    summed[:, :width] = low[:, :width].astype(bf16)
    summed[:, width : 3 * width] = (low[:, width:] + high[:, : 2 * width]).astype(bf16)
    summed[:, 3 * width :] = high[:, 2 * width :].astype(bf16)


def targets_body(own, below, above, targets):
    _, _, shared = grid_place()
    width = own.shape[1]
    targets[:, :width] = jnp.where(shared[2], below[...], jnp.zeros_like(below))
    targets[:, width : 2 * width] = own[...]
    targets[:, 2 * width :] = jnp.where(shared[3], above[...], jnp.zeros_like(above))


def inverse_body(*refs, coarse_dofs):
    *parts, operator = refs
    _, col, _ = grid_place()
    width = len(parts) * coarse_dofs
    edge = jnp.zeros((width, operator.shape[1]), bf16)
    operator[:width, :] = edge
    operator[operator.shape[0] - width :, :] = edge
    for index in range(parts[0].shape[0] // coarse_dofs):
        for flip, part in enumerate(parts):
            start = (index + 1) * width + (col ^ flip) * coarse_dofs
            rows = pl.ds(pl.multiple_of(start, coarse_dofs), coarse_dofs)
            operator[rows, :] = part[index * coarse_dofs : (index + 1) * coarse_dofs, :]


def coarse_body(*refs):
    *rows, operator, solved = refs
    depth = rows[0].shape[1]
    row, _, _ = grid_place()
    total = None
    for step, block in enumerate(rows):
        pair = lax.rem(row // 2 - step + len(rows), len(rows))
        sources = pl.ds(pl.multiple_of(pair * (depth // 2), depth // 2), depth)
        part = jnp.dot(block[...], operator[sources, :], preferred_element_type=f32)
        total = part if total is None else total + part
    solved[...] = total.astype(bf16)


def correct_body(*refs, cells, parts):
    solved = refs[:parts]
    turned, local_part, weighted, *faces, whole = refs[parts:]
    _, col, shared = grid_place()
    size = solved[0].shape[0]
    for flip, part in enumerate(solved):
        whole[pl.ds(pl.multiple_of((col ^ flip) * size, size), size), :] = part[...]
    for side in range(4):
        rows = slice(side * cells, (side + 1) * cells)
        coarse_part = lax.dot_general(
            turned[rows, :], whole[...], (((1,), (1,)), ((), ())), preferred_element_type=f32
        )
        weighted[rows, :] = weight_of(shared[side]) * (local_part[rows, :] + coarse_part)
    put_faces(weighted, faces, cells)


def schur_body(
    mask, weighted, w, e, s, n, schur, loads, moved, value, o1, o2, o3, o4, low, *, cells
):
    received = (w, e, s, n)
    for side in range(4):
        rows = slice(side * cells, (side + 1) * cells)
        moved[rows, :] = damping * assembled(side, weighted[rows, :], received, mask, rows)
        low[rows, :] = moved[rows, :].astype(bf16)
    value[...] = loads[...] - jnp.dot(schur[...], low[...], preferred_element_type=f32)
    put_faces(value, (o1, o2, o3, o4), cells)


def final_body(mask, weighted, w, e, s, n, before, moved, *, cells):
    received = (w, e, s, n)
    for side in range(4):
        rows = slice(side * cells, (side + 1) * cells)
        total = assembled(side, weighted[rows, :], received, mask, rows)
        moved[rows, :] = before[rows, :] + damping * total


def wide_plan(loads, schur, local_inverse, basis, coarse_inverse, face_len):
    local_dofs = loads.shape[2]
    load_cases = loads.shape[3]
    cells = local_dofs // 4
    coarse_dofs = basis.shape[2] // 9
    row_count = lax.axis_size("fx")
    col_count = lax.axis_size("fy")
    width = col_count * coarse_dofs
    slice_cases = load_cases // col_count
    local_load = loads[0, 0]
    array = jax.ShapeDtypeStruct
    vector32 = array((local_dofs, load_cases), f32)
    vector16 = array((local_dofs, load_cases), bf16)
    face16 = [array((cells, load_cases), bf16)] * 4
    row16 = array((slice_cases, 3 * width), bf16)
    flips = range(1, col_count)
    steps = range(1, row_count // 2)

    def exchange(faces):
        west, east, south, north = faces
        return (
            shift(east, "fy", 1),
            shift(west, "fy", -1),
            shift(north, "fx", 1),
            shift(south, "fx", -1),
        )

    own = coarse_inverse.reshape(row_count * coarse_dofs, width)
    below = shift(own, "fx", 1)
    above = shift(own, "fx", -1)

    *faces, mask = local_kernel(
        faces_body,
        face16 + [array((local_dofs, 128), f32)],
        local_dofs * load_cases,
        face_len.reshape(4),
        local_load,
    )
    received = exchange(faces)

    framed, turned = local_kernel(
        functools.partial(basis_body, coarse_dofs=coarse_dofs, col_count=col_count),
        [array((3 * width, local_dofs), bf16), array((local_dofs, 3 * width), bf16)],
        8 * width * local_dofs,
        basis[0, 0],
    )
    (targets,) = local_kernel(
        targets_body,
        [array((row_count * coarse_dofs, 3 * width), bf16)],
        8 * width * width,
        own,
        below,
        above,
    )

    def project(value, received):
        return local_kernel(
            functools.partial(pieces_body, cells=cells),
            [vector16] + [row16] * col_count,
            2 * local_dofs * load_cases * 3 * width,
            mask,
            value,
            *received,
            framed,
            scratch=[pltpu.VMEM((load_cases, 3 * width), bf16)],
        )

    def restrict(parts):
        total = parts[0].astype(f32)
        for flip in flips:
            total = total + swap(parts[flip], "fy", flip).astype(f32)
        total = total.astype(bf16)
        (pair_sum,) = local_kernel(
            pair_body,
            [array((slice_cases, 4 * width), bf16)],
            4 * slice_cases * width,
            total,
            swap(total, "fx", 1),
        )
        return [pair_sum] + [shift(pair_sum, "fx", 2 * k) for k in steps]

    def correct(rows, scaled, operator):
        local_part = jnp.dot(local_inverse[0, 0], scaled, preferred_element_type=f32)
        (solved,) = local_kernel(
            coarse_body, [row16], 12 * slice_cases * width * width * row_count, *rows, operator
        )
        solved = [solved] + [swap(solved, "fy", k) for k in flips]
        weighted, *faces = local_kernel(
            functools.partial(correct_body, cells=cells, parts=col_count),
            [vector32] + face16,
            2 * local_dofs * load_cases * 3 * width,
            *solved,
            turned,
            local_part,
            scratch=[pltpu.VMEM((load_cases, 3 * width), bf16)],
        )
        return weighted, exchange(faces)

    scaled, *parts = project(local_load, received)
    rows = restrict(parts)
    (operator,) = local_kernel(
        functools.partial(inverse_body, coarse_dofs=coarse_dofs),
        [array(((row_count + 2) * width, 3 * width), bf16)],
        4 * row_count * width * width,
        targets,
        *[swap(targets, "fy", k) for k in flips],
    )
    weighted, received = correct(rows, scaled, operator)
    moved, value, *faces = local_kernel(
        functools.partial(schur_body, cells=cells),
        [vector32, vector32] + face16,
        2 * local_dofs * local_dofs * load_cases,
        mask,
        weighted,
        *received,
        schur[0, 0],
        local_load,
        scratch=[pltpu.VMEM((local_dofs, load_cases), bf16)],
    )
    scaled, *parts = project(value, exchange(faces))
    weighted, received = correct(restrict(parts), scaled, operator)
    (moved,) = local_kernel(
        functools.partial(final_body, cells=cells),
        [vector32],
        8 * local_dofs * load_cases,
        mask,
        weighted,
        *received,
        moved,
    )
    return moved.reshape(1, 1, local_dofs, load_cases)


def is_wide(row_count, col_count, coarse_dofs):
    width = col_count * coarse_dofs
    return row_count * width * 9 * width * 2 <= wide_limit


def solution(mesh):
    placed = (
        P("fx", "fy", None, None),
        P("fx", "fy", None, None),
        P("fx", "fy", None, None),
        P("fx", "fy", None, None),
        P(None, "fy", None, "fx"),
        P("fx", "fy", None),
    )

    def sharded(body):
        return jax.shard_map(
            body,
            mesh=mesh,
            in_specs=placed,
            out_specs=P("fx", "fy", None, None),
            check_vma=False,
        )

    def whole(*args):
        basis = args[3]
        if not is_wide(mesh.shape["fx"], mesh.shape["fy"], basis.shape[2] // 9):
            return sharded(narrow_plan)(*args)

        return sharded(wide_plan)(*args)

    return whole
```
